64 devices in a mesh: rep: 8 (over x, y, core), dp: 8 (over z).
Axes of the slice: x: 2, y: 2, z: 8, core: 2. Of those that a mesh axis runs over, the one named last changes fastest.
The devices are a block of a 4x4x8 slice.
Arguments:
- g_w_gate: bfloat16 [64, 2, 512, 1280], P(('rep', 'dp')), parts along dimension 0
- g_w_up: bfloat16 [64, 2, 512, 1280], P(('rep', 'dp')), parts along dimension 0
- g_w_down: bfloat16 [64, 2, 1280, 512], P(('rep', 'dp')), parts along dimension 0
- w_gate: bfloat16 [2, 512, 1280], replicated
- w_up: bfloat16 [2, 512, 1280], replicated
- w_down: bfloat16 [2, 1280, 512], replicated
- m_w_gate: float32 [2, 512, 1280], P(None, 'dp')
- m_w_up: float32 [2, 512, 1280], P(None, 'dp')
- m_w_down: float32 [2, 1280, 512], P(None, 'dp')
- v_w_gate: float32 [2, 512, 1280], P(None, 'dp')
- v_w_up: float32 [2, 512, 1280], P(None, 'dp')
- v_w_down: float32 [2, 1280, 512], P(None, 'dp')
Outputs:
- output 1: bfloat16 [16, 512, 1280], P('rep'), parts along dimension 0
- output 2: bfloat16 [16, 512, 1280], P('rep'), parts along dimension 0
- output 3: bfloat16 [16, 1280, 512], P('rep'), parts along dimension 0
- output 4: float32 [16, 512, 1280], P('rep', 'dp'), parts along dimension 0
- output 5: float32 [16, 512, 1280], P('rep', 'dp'), parts along dimension 0
- output 6: float32 [16, 1280, 512], P('rep', 'dp'), parts along dimension 0
- output 7: float32 [16, 512, 1280], P('rep', 'dp'), parts along dimension 0
- output 8: float32 [16, 512, 1280], P('rep', 'dp'), parts along dimension 0
- output 9: float32 [16, 1280, 512], P('rep', 'dp'), parts along dimension 0
There are 8 independent parts. The reference program is written for one: setup_inputs(seed, part) draws one part's arguments, and reference() takes and returns one part's arrays. A program takes and returns all parts, laid end to end along the dimension named above; an argument that names none is the same for every part.
All inputs are finite; a program needn't handle non-finite values.
Results may differ from the reference program's by a relative error of at most 0.022.
Values are sent between devices in bfloat16 or wider.
A program may use at most 768 MiB of HBM per device.

```python
import jax
import jax.numpy as jnp
from jax import lax

DEVICES = 8
D = 512
FF = 1280
LAYERS = 2
NAMES = ("w_gate", "w_up", "w_down")
SHAPES = {"w_gate": (LAYERS, D, FF), "w_up": (LAYERS, D, FF), "w_down": (LAYERS, FF, D)}


def setup_inputs(seed: int = 0, part: int = 0) -> dict:
    kz, *keys = jax.random.split(jax.random.key(seed), 1 + 5 * len(NAMES))
    loud = 2.0 ** jax.random.uniform(kz, (), jnp.float32, -1.0, 1.0)
    drawn = {}
    for name, key, both in zip(NAMES, keys[:3], keys[3:6], strict=True):
        own = jax.random.normal(jax.random.fold_in(key, part), (DEVICES, *SHAPES[name]), jnp.float32)
        shared = jax.random.normal(jax.random.fold_in(both, part), SHAPES[name], jnp.float32)
        drawn["g_" + name] = (loud * (0.7 * shared / DEVICES + 0.7 * own * DEVICES**-0.5)).astype(jnp.bfloat16)
    for name, key in zip(NAMES, keys[6:9], strict=True):
        drawn[name] = (jax.random.normal(key, SHAPES[name], jnp.float32) * SHAPES[name][1] ** -0.5).astype(jnp.bfloat16)
    for name, key in zip(NAMES, keys[9:12], strict=True):
        drawn["m_" + name] = loud * 0.5 * jax.random.normal(key, SHAPES[name], jnp.float32)
    for name, key in zip(NAMES, keys[12:15], strict=True):
        drawn["v_" + name] = loud * loud * jax.random.uniform(key, SHAPES[name], jnp.float32, 0.5, 1.5)
    return drawn


def adamw(w, m, v, g):
    m = 0.9 * m + 0.1 * g
    v = 0.95 * v + 0.05 * g * g
    step = m * lax.rsqrt(v + 1e-8) + 0.1 * w
    return (w - 0.02 * step).astype(jnp.bfloat16), m, v


def clipped(gradients, sum_of_squares, count):
    factor = jnp.minimum(1.0, 0.5 * lax.rsqrt(sum_of_squares / count + 1e-30))
    return [g * factor for g in gradients]


def reference(g_w_gate, g_w_up, g_w_down, w_gate, w_up, w_down, m_w_gate, m_w_up, m_w_down, v_w_gate, v_w_up, v_w_down):
    def total(terms):
        return lax.scan(lambda so_far, term: (so_far + term.astype(jnp.float32), None), jnp.zeros(terms.shape[1:], jnp.float32), terms)[0]

    gradients = [total(terms).astype(jnp.bfloat16).astype(jnp.float32) for terms in (g_w_gate, g_w_up, g_w_down)]
    gradients = clipped(gradients, sum(jnp.sum(g * g) for g in gradients), sum(g.size for g in gradients))
    new = [
        adamw(w.astype(jnp.float32), m, v, g)
        for w, m, v, g in zip((w_gate, w_up, w_down), (m_w_gate, m_w_up, m_w_down), (v_w_gate, v_w_up, v_w_down), gradients, strict=True)
    ]
    return tuple(one[which] for which in range(3) for one in new)
```

```python
import functools

import jax
import jax.numpy as jnp
from jax import lax
from jax.experimental import pallas as pl
from jax.experimental.pallas import tpu as pltpu
from jax.sharding import PartitionSpec as P

MESH = pl.DeviceIdType.MESH
F32, BF16 = jnp.float32, jnp.bfloat16
ROWS, LANES = 16, 256


def kernel(n, *refs):
    terms, weights, m_in, v_in = (refs[i : i + 3] for i in (0, 3, 6, 9))
    w_out, m_out, v_out = (refs[i : i + 3] for i in (12, 15, 18))
    own, arrived, total, w_old, w_new, m, v = (refs[i : i + 3] for i in (21, 24, 27, 30, 33, 36, 39))
    squares, load_sem, state_sem, out_sem, rs_send, rs_recv, sq_send, sq_recv, ag_send, ag_recv = refs[42:]

    half = n // 2
    me = lax.axis_index("dp")
    rows = [ref.shape[1] for ref in m_in]
    cols = [ref.shape[2] for ref in m_in]
    count = n * sum(2 * r * c for r, c in zip(rows, cols, strict=True))

    def at(offset):
        return lax.rem(me + offset + n, n)

    def block(weight, offset):
        return pl.multiple_of(at(offset) * rows[weight], rows[weight])

    def load(weight, offset):
        part = pl.ds(block(weight, offset), rows[weight])
        return pltpu.make_async_copy(terms[weight].at[:, part], own[weight].at[:, part], load_sem.at[weight, offset % n])

    order = [half]
    for distance in range(half - 1, 0, -1):
        order += [distance, -distance]
    order += [0]
    for offset in order:
        for weight in range(3):
            load(weight, offset).start()

    def state(which, weight):
        if which == 0:
            return pltpu.make_async_copy(weights[weight].at[:, pl.ds(block(weight, 0), rows[weight])], w_old[weight], state_sem.at[0, weight])
        source, target = ((m_in, m), (v_in, v))[which - 1]
        return pltpu.make_async_copy(source[weight], target[weight], state_sem.at[which, weight])

    for which in range(3):
        for weight in range(3):
            state(which, weight).start()

    barrier = pltpu.get_barrier_semaphore()
    for offset in (1, -1):
        pl.semaphore_signal(barrier, inc=1, device_id={"dp": at(offset)}, device_id_type=MESH)
    pl.semaphore_wait(barrier, 2)

    sign = (1, -1)
    sends = n - 1

    def distance(k):
        return half - (k + 1) // 2

    def layer(way, k):
        return (way + k) % 2

    def send_sum(way, k, weight):
        if k < 2:
            source = own[weight].at[layer(way, k), pl.ds(block(weight, sign[way] * distance(k)), rows[weight])]
        else:
            source = arrived[weight].at[way, k - 2]
        return pltpu.make_async_remote_copy(
            src_ref=source,
            dst_ref=arrived[weight].at[way, k],
            send_sem=rs_send.at[way, k, weight],
            recv_sem=rs_recv.at[way, k, weight],
            device_id={"dp": at(sign[way])},
            device_id_type=MESH,
        )

    loaded = set()

    def need(weight, offset):
        if (weight, offset % n) not in loaded:
            loaded.add((weight, offset % n))
            load(weight, offset).wait()

    for k in range(2):
        for weight in range(3):
            for way in range(2):
                need(weight, sign[way] * distance(k))
                send_sum(way, k, weight).start()

    def pieces(weight, body, carry=None):
        def step(i, carry):
            r = pl.multiple_of(i * ROWS, ROWS)
            for c in range(0, cols[weight], LANES):
                carry = body(r, pl.ds(c, LANES), carry)
            return carry

        return lax.fori_loop(0, rows[weight] // ROWS, step, carry)

    def add(way, k, weight):
        offset, which = sign[way] * (distance(k) - 1), layer(way, k)
        base = block(weight, offset)

        def body(r, c, carry):
            term = own[weight][which, pl.ds(pl.multiple_of(base + r, ROWS), ROWS), c].astype(F32)
            so_far = arrived[weight][way, k, pl.ds(r, ROWS), c].astype(F32)
            arrived[weight][way, k, pl.ds(r, ROWS), c] = (so_far + term).astype(BF16)
            return carry

        pieces(weight, body, 0)

    for k in range(sends - 2):
        for weight in range(3):
            for way in range(2):
                need(weight, sign[way] * (distance(k) - 1))
                send_sum(way, k, weight).wait_recv()
                add(way, k, weight)
                send_sum(way, k + 2, weight).start()

    def finish(which, weight, sums):
        base = block(weight, 0)
        first, second = ((way, k) for way in range(2) for k in (sends - 2, sends - 1) if layer(way, k) == which)

        def body(r, c, sums):
            g = own[weight][which, pl.ds(pl.multiple_of(base + r, ROWS), ROWS), c].astype(F32)
            g += arrived[weight][first[0], first[1], pl.ds(r, ROWS), c].astype(F32)
            g += arrived[weight][second[0], second[1], pl.ds(r, ROWS), c].astype(F32)
            g = g.astype(BF16)
            total[weight][which, pl.ds(r, ROWS), c] = g
            g = g.astype(F32)
            g = g * g
            return sums + (g[:8] + g[8:])

        return pieces(weight, body, sums)

    for weight in range(3):
        need(weight, 0)
        for way in range(2):
            send_sum(way, sends - 2, weight).wait_recv()
    sums = jnp.zeros((8, LANES), F32)
    for weight in range(3):
        for way in range(2):
            send_sum(way, sends - 1, weight).wait_recv()
            sums = finish(layer(way, sends - 1), weight, sums)
    sums = sum(sums[:, c : c + 128] for c in range(0, LANES, 128))
    squares[0] = jnp.broadcast_to(jnp.sum(sums, axis=0, keepdims=True), (8, 128))

    def send_squares(offset):
        return pltpu.make_async_remote_copy(
            src_ref=squares.at[0],
            dst_ref=squares.at[offset],
            send_sem=sq_send.at[offset],
            recv_sem=sq_recv.at[offset],
            device_id={"dp": at(offset)},
            device_id_type=MESH,
        )

    far_first = sorted(range(1, n), key=lambda offset: -min(offset, n - offset))
    for offset in far_first:
        send_squares(offset).start()
    for which in range(3):
        for weight in range(3):
            state(which, weight).wait()
    everyone = squares[0, :1]
    for offset in reversed(far_first):
        send_squares(offset).wait_recv()
        everyone += squares[offset, :1]
    everyone = jnp.sum(everyone, axis=1, keepdims=True)
    factor = jnp.minimum(1.0, 0.5 * lax.rsqrt(everyone / count + 1e-30))

    def adamw(which, weight):
        def body(r, c, carry):
            part = (which, pl.ds(r, ROWS), c)
            g = total[weight][part].astype(F32) * factor
            w = w_old[weight][part].astype(F32)
            m_new = 0.9 * m[weight][part] + 0.1 * g
            v_new = 0.95 * v[weight][part] + 0.05 * g * g
            m[weight][part] = m_new
            v[weight][part] = v_new
            step = m_new * lax.rsqrt(v_new + 1e-8) + 0.1 * w
            w_new[weight][part] = (w - 0.02 * step).astype(BF16)
            return carry

        pieces(weight, body, 0)

    def send_new(way, q, which, weight):
        part = pl.ds(block(weight, -sign[way] * q), rows[weight])
        place = w_out[weight].at[which, part]
        return pltpu.make_async_remote_copy(
            src_ref=w_new[weight].at[which] if q == 0 else place,
            dst_ref=place,
            send_sem=ag_send.at[way, q, which, weight],
            recv_sem=ag_recv.at[way, q, which, weight],
            device_id={"dp": at(sign[way])},
            device_id_type=MESH,
        )

    def recv_new(way, q, which, weight):
        part = pl.ds(block(weight, -sign[way] * (q + 1)), rows[weight])
        place = w_out[weight].at[which, part]
        return pltpu.make_async_remote_copy(
            src_ref=place,
            dst_ref=place,
            send_sem=ag_send.at[way, q, which, weight],
            recv_sem=ag_recv.at[way, q, which, weight],
            device_id={"dp": at(sign[way])},
            device_id_type=MESH,
        )

    def keep(which, weight, what):
        if what == 0:
            part = pl.ds(block(weight, 0), rows[weight])
            return pltpu.make_async_copy(w_new[weight].at[which], w_out[weight].at[which, part], out_sem.at[0, which, weight])
        source, target = ((m, m_out), (v, v_out))[what - 1]
        return pltpu.make_async_copy(source[weight].at[which], target[weight].at[which], out_sem.at[what, which, weight])

    for which in range(2):
        for weight in range(3):
            adamw(which, weight)
            for way in range(2):
                send_new(way, 0, which, weight).start()
            for what in range(3):
                keep(which, weight, what).start()
    for q in range(half):
        for which in range(2):
            for weight in range(3):
                for way in range(2):
                    if q == half - 1 and which != way:
                        continue
                    recv_new(way, q, which, weight).wait_recv()
                    if q + 1 < half - 1 or (q + 1 == half - 1 and which == way):
                        send_new(way, q + 1, which, weight).start()

    for weight in range(3):
        for way in range(2):
            for k in range(sends):
                send_sum(way, k, weight).wait_send()
            for q in range(half):
                for which in range(2):
                    if q < half - 1 or which == way:
                        send_new(way, q, which, weight).wait_send()
        for which in range(2):
            for what in range(3):
                keep(which, weight, what).wait()
    for offset in far_first:
        send_squares(offset).wait_send()


def solution(mesh):
    n = mesh.shape["dp"]

    def step(*arrays):
        terms, weights, m, v = (arrays[i : i + 3] for i in (0, 3, 6, 9))
        terms = tuple(t[0] for t in terms)
        half = n // 2
        shapes = [one.shape for one in m]
        dma = pltpu.SemaphoreType.DMA
        out = [jax.ShapeDtypeStruct(w.shape, w.dtype) for w in weights]
        out += [jax.ShapeDtypeStruct(one.shape, one.dtype) for one in (*m, *v)]
        scratch = [pltpu.VMEM(t.shape, t.dtype) for t in terms]
        scratch += [pltpu.VMEM((2, n - 1, *s[1:]), BF16) for s in shapes]
        scratch += [pltpu.VMEM(s, BF16) for _ in range(3) for s in shapes]
        scratch += [pltpu.VMEM(s, F32) for _ in range(2) for s in shapes]
        scratch += [
            pltpu.VMEM((n, 8, 128), F32),
            dma((3, n)),
            dma((3, 3)),
            dma((3, 2, 3)),
            dma((2, n - 1, 3)),
            dma((2, n - 1, 3)),
            dma((n,)),
            dma((n,)),
            dma((2, half, 2, 3)),
            dma((2, half, 2, 3)),
        ]
        return pl.pallas_call(
            functools.partial(kernel, n),
            out_shape=out,
            in_specs=[pl.BlockSpec(memory_space=pltpu.HBM)] * 12,
            out_specs=[pl.BlockSpec(memory_space=pl.ANY)] * 9,
            scratch_shapes=scratch,
            compiler_params=pltpu.CompilerParams(collective_id=0, has_side_effects=True, vmem_limit_bytes=40 * 2**20),
        )(*terms, *weights, *m, *v)

    all_of, cut = P(None, None, None), P(None, "dp", None)
    return jax.shard_map(
        step,
        mesh=mesh,
        in_specs=(P(("rep", "dp"), None, None, None),) * 3 + (all_of,) * 3 + (cut,) * 6,
        out_specs=(P("rep", None, None),) * 3 + (P("rep", "dp", None),) * 6,
        check_vma=False,
    )
```

```python
import functools

import jax
import jax.numpy as jnp
from jax import lax
from jax.experimental import pallas as pl
from jax.experimental.pallas import tpu as pltpu
from jax.sharding import PartitionSpec as P

MESH = pl.DeviceIdType.MESH
F32, BF16 = jnp.float32, jnp.bfloat16
ROWS, LANES = 16, 256


def kernel(n, *refs):
    terms, weights, m_in, v_in = (refs[i : i + 3] for i in (0, 3, 6, 9))
    w_out, m_out, v_out = (refs[i : i + 3] for i in (12, 15, 18))
    own, arrived, total, w_old, m, v = (refs[i : i + 3] for i in (21, 24, 27, 30, 33, 36))
    squares, load_sem, state_sem, rs_send, rs_recv, sq_send, sq_recv, ag_send, ag_recv = refs[39:]

    half = n // 2
    me = lax.axis_index("dp")
    rows = [ref.shape[1] for ref in m_in]
    cols = [ref.shape[2] for ref in m_in]
    count = n * sum(2 * r * c for r, c in zip(rows, cols, strict=True))

    def at(offset):
        return lax.rem(me + offset + n, n)

    def block(weight, offset):
        return pl.multiple_of(at(offset) * rows[weight], rows[weight])

    def load(weight, offset):
        part = pl.ds(block(weight, offset), rows[weight])
        return pltpu.make_async_copy(terms[weight].at[:, part], own[weight].at[:, part], load_sem.at[weight, offset % n])

    order = [half]
    for distance in range(half - 1, 0, -1):
        order += [distance, -distance]
    order += [0]
    for offset in order:
        for weight in range(3):
            load(weight, offset).start()

    def state(which, weight):
        if which == 0:
            return pltpu.make_async_copy(weights[weight].at[:, pl.ds(block(weight, 0), rows[weight])], w_old[weight], state_sem.at[0, weight])
        source, target = ((m_in, m), (v_in, v))[which - 1]
        return pltpu.make_async_copy(source[weight], target[weight], state_sem.at[which, weight])

    for which in range(3):
        for weight in range(3):
            state(which, weight).start()

    barrier = pltpu.get_barrier_semaphore()
    for offset in (1, -1):
        pl.semaphore_signal(barrier, inc=1, device_id={"dp": at(offset)}, device_id_type=MESH)
    pl.semaphore_wait(barrier, 2)

    sign = (1, -1)
    sends = n - 1

    def distance(k):
        return half - (k + 1) // 2

    def layer(way, k):
        return (way + k) % 2

    def send_sum(way, k, weight):
        if k < 2:
            source = own[weight].at[layer(way, k), pl.ds(block(weight, sign[way] * distance(k)), rows[weight])]
        else:
            source = arrived[weight].at[way, k - 2]
        return pltpu.make_async_remote_copy(
            src_ref=source,
            dst_ref=arrived[weight].at[way, k],
            send_sem=rs_send.at[way, k, weight],
            recv_sem=rs_recv.at[way, k, weight],
            device_id={"dp": at(sign[way])},
            device_id_type=MESH,
        )

    loaded = set()

    def need(weight, offset):
        if (weight, offset % n) not in loaded:
            loaded.add((weight, offset % n))
            load(weight, offset).wait()

    for k in range(2):
        for weight in range(3):
            for way in range(2):
                need(weight, sign[way] * distance(k))
                send_sum(way, k, weight).start()

    def pieces(weight, body, carry=None):
        def step(i, carry):
            r = pl.multiple_of(i * ROWS, ROWS)
            for c in range(0, cols[weight], LANES):
                carry = body(r, pl.ds(c, LANES), carry)
            return carry

        return lax.fori_loop(0, rows[weight] // ROWS, step, carry)

    def add(way, k, weight):
        offset, which = sign[way] * (distance(k) - 1), layer(way, k)
        base = block(weight, offset)

        def body(r, c, carry):
            term = own[weight][which, pl.ds(pl.multiple_of(base + r, ROWS), ROWS), c].astype(F32)
            so_far = arrived[weight][way, k, pl.ds(r, ROWS), c].astype(F32)
            arrived[weight][way, k, pl.ds(r, ROWS), c] = (so_far + term).astype(BF16)
            return carry

        pieces(weight, body, 0)

    for k in range(sends - 2):
        for weight in range(3):
            for way in range(2):
                need(weight, sign[way] * (distance(k) - 1))
                send_sum(way, k, weight).wait_recv()
                add(way, k, weight)
                send_sum(way, k + 2, weight).start()

    def finish(which, weight, sums):
        base = block(weight, 0)
        first, second = ((way, k) for way in range(2) for k in (sends - 2, sends - 1) if layer(way, k) == which)

        def body(r, c, sums):
            g = own[weight][which, pl.ds(pl.multiple_of(base + r, ROWS), ROWS), c].astype(F32)
            g += arrived[weight][first[0], first[1], pl.ds(r, ROWS), c].astype(F32)
            g += arrived[weight][second[0], second[1], pl.ds(r, ROWS), c].astype(F32)
            g = g.astype(BF16)
            total[weight][which, pl.ds(r, ROWS), c] = g
            g = g.astype(F32)
            g = g * g
            return sums + (g[:8] + g[8:])

        return pieces(weight, body, sums)

    for weight in range(3):
        need(weight, 0)
        for way in range(2):
            send_sum(way, sends - 2, weight).wait_recv()
    sums = jnp.zeros((8, LANES), F32)
    for weight in range(3):
        for way in range(2):
            send_sum(way, sends - 1, weight).wait_recv()
            sums = finish(layer(way, sends - 1), weight, sums)
    sums = sum(sums[:, c : c + 128] for c in range(0, LANES, 128))
    squares[0] = jnp.broadcast_to(jnp.sum(sums, axis=0, keepdims=True), (8, 128))

    def send_squares(offset):
        return pltpu.make_async_remote_copy(
            src_ref=squares.at[0],
            dst_ref=squares.at[offset],
            send_sem=sq_send.at[offset],
            recv_sem=sq_recv.at[offset],
            device_id={"dp": at(offset)},
            device_id_type=MESH,
        )

    far_first = sorted(range(1, n), key=lambda offset: -min(offset, n - offset))
    for offset in far_first:
        send_squares(offset).start()
    for which in range(3):
        for weight in range(3):
            state(which, weight).wait()
    everyone = squares[0, :1]
    for offset in reversed(far_first):
        send_squares(offset).wait_recv()
        everyone += squares[offset, :1]
    everyone = jnp.sum(everyone, axis=1, keepdims=True)
    factor = jnp.minimum(1.0, 0.5 * lax.rsqrt(everyone / count + 1e-30))

    def adamw(which, weight):
        base = block(weight, 0)

        def body(r, c, carry):
            part = (which, pl.ds(r, ROWS), c)
            g = total[weight][part].astype(F32) * factor
            w = w_old[weight][part].astype(F32)
            m_new = 0.9 * m[weight][part] + 0.1 * g
            v_new = 0.95 * v[weight][part] + 0.05 * g * g
            m_out[weight][part] = m_new
            v_out[weight][part] = v_new
            step = m_new * lax.rsqrt(v_new + 1e-8) + 0.1 * w
            w_out[weight][which, pl.ds(pl.multiple_of(base + r, ROWS), ROWS), c] = (w - 0.02 * step).astype(BF16)
            return carry

        pieces(weight, body, 0)

    def send_new(way, q, which, weight):
        part = pl.ds(block(weight, -sign[way] * q), rows[weight])
        place = w_out[weight].at[which, part]
        return pltpu.make_async_remote_copy(
            src_ref=place,
            dst_ref=place,
            send_sem=ag_send.at[way, q, which, weight],
            recv_sem=ag_recv.at[way, q, which, weight],
            device_id={"dp": at(sign[way])},
            device_id_type=MESH,
        )

    def recv_new(way, q, which, weight):
        part = pl.ds(block(weight, -sign[way] * (q + 1)), rows[weight])
        place = w_out[weight].at[which, part]
        return pltpu.make_async_remote_copy(
            src_ref=place,
            dst_ref=place,
            send_sem=ag_send.at[way, q, which, weight],
            recv_sem=ag_recv.at[way, q, which, weight],
            device_id={"dp": at(sign[way])},
            device_id_type=MESH,
        )

    for which in range(2):
        for weight in range(3):
            adamw(which, weight)
            for way in range(2):
                send_new(way, 0, which, weight).start()
    for q in range(half):
        for which in range(2):
            for weight in range(3):
                for way in range(2):
                    if q == half - 1 and which != way:
                        continue
                    recv_new(way, q, which, weight).wait_recv()
                    if q + 1 < half - 1 or (q + 1 == half - 1 and which == way):
                        send_new(way, q + 1, which, weight).start()

    for weight in range(3):
        for way in range(2):
            for k in range(sends):
                send_sum(way, k, weight).wait_send()
            for q in range(half):
                for which in range(2):
                    if q < half - 1 or which == way:
                        send_new(way, q, which, weight).wait_send()
    for offset in far_first:
        send_squares(offset).wait_send()


def put_out(*refs):
    arrays = len(refs) // 2
    sem = refs[-1]
    copies = [pltpu.make_async_copy(refs[i].at[half], refs[arrays + i].at[half], sem.at[i, half]) for i in range(arrays) for half in range(2)]
    for copy in copies:
        copy.start()
    for copy in copies:
        copy.wait()


def solution(mesh):
    n = mesh.shape["dp"]

    def step(*arrays):
        terms, weights, m, v = (arrays[i : i + 3] for i in (0, 3, 6, 9))
        terms = tuple(t[0] for t in terms)
        half = n // 2
        shapes = [one.shape for one in m]
        dma = pltpu.SemaphoreType.DMA
        out = [jax.ShapeDtypeStruct(w.shape, w.dtype) for w in weights]
        out += [jax.ShapeDtypeStruct(one.shape, one.dtype) for one in (*m, *v)]
        scratch = [pltpu.VMEM(t.shape, t.dtype) for t in terms]
        scratch += [pltpu.VMEM((2, n - 1, *s[1:]), BF16) for s in shapes]
        scratch += [pltpu.VMEM(s, BF16) for _ in range(2) for s in shapes]
        scratch += [pltpu.VMEM(s, F32) for _ in range(2) for s in shapes]
        scratch += [
            pltpu.VMEM((n, 8, 128), F32),
            dma((3, n)),
            dma((3, 3)),
            dma((2, n - 1, 3)),
            dma((2, n - 1, 3)),
            dma((n,)),
            dma((n,)),
            dma((2, half, 2, 3)),
            dma((2, half, 2, 3)),
        ]
        in_hbm = [pltpu.with_memory_space_constraint(one, pltpu.HBM) for one in (*terms, *weights, *m, *v)]
        new = pl.pallas_call(
            functools.partial(kernel, n),
            out_shape=[pltpu.VMEM(one.shape, one.dtype) for one in out],
            in_specs=[pl.BlockSpec(memory_space=pltpu.HBM)] * len(in_hbm),
            out_specs=[pl.BlockSpec(memory_space=pltpu.VMEM)] * len(out),
            scratch_shapes=scratch,
            compiler_params=pltpu.CompilerParams(collective_id=0, has_side_effects=True, vmem_limit_bytes=28 * 2**20),
        )(*in_hbm)
        return pl.pallas_call(
            put_out,
            out_shape=out,
            in_specs=[pl.BlockSpec(memory_space=pltpu.VMEM)] * len(out),
            out_specs=[pl.BlockSpec(memory_space=pl.ANY)] * len(out),
            scratch_shapes=[dma((len(out), 2))],
            compiler_params=pltpu.CompilerParams(vmem_limit_bytes=2**20),
        )(*(pltpu.with_memory_space_constraint(one, pltpu.VMEM) for one in new))

    all_of, cut = P(None, None, None), P(None, "dp", None)
    return jax.shard_map(
        step,
        mesh=mesh,
        in_specs=(P(("rep", "dp"), None, None, None),) * 3 + (all_of,) * 3 + (cut,) * 6,
        out_specs=(P("rep", None, None),) * 3 + (P("rep", "dp", None),) * 6,
        check_vma=False,
    )
```

```python
import functools

import jax
import jax.numpy as jnp
from jax import lax
from jax.experimental import pallas as pl
from jax.experimental.pallas import tpu as pltpu
from jax.sharding import PartitionSpec as P

MESH = pl.DeviceIdType.MESH
F32, BF16 = jnp.float32, jnp.bfloat16
ROWS, LANES = 16, 256

LATE, HEAD_START_NS = 0, 13000


def reduce_and_step(n, *refs):
    terms, weights, m_in, v_in = (refs[i : i + 3] for i in (0, 3, 6, 9))
    w_out, m_out, v_out = (refs[i : i + 3] for i in (12, 15, 18))
    own, arrived, total, w_old, m, v = (refs[i : i + 3] for i in (21, 24, 27, 30, 33, 36))
    squares, load_sem, state_sem, rs_send, rs_recv, sq_send, sq_recv = refs[39:]

    half = n // 2
    me = lax.axis_index("dp")
    rows = [ref.shape[1] for ref in m_in]
    cols = [ref.shape[2] for ref in m_in]
    count = n * sum(2 * r * c for r, c in zip(rows, cols, strict=True))

    def at(offset):
        return lax.rem(me + offset + n, n)

    def block(weight, offset):
        return pl.multiple_of(at(offset) * rows[weight], rows[weight])

    def load(weight, offset):
        part = pl.ds(block(weight, offset), rows[weight])
        return pltpu.make_async_copy(terms[weight].at[:, part], own[weight].at[:, part], load_sem.at[weight, offset % n])

    order = [half]
    for distance in range(half - 1, 0, -1):
        order += [distance, -distance]
    order += [0]
    for offset in order:
        for weight in range(3):
            load(weight, offset).start()

    def state(which, weight):
        if which == 0:
            return pltpu.make_async_copy(weights[weight].at[:, pl.ds(block(weight, 0), rows[weight])], w_old[weight], state_sem.at[0, weight])
        source, target = ((m_in, m), (v_in, v))[which - 1]
        return pltpu.make_async_copy(source[weight], target[weight], state_sem.at[which, weight])

    for which in range(3):
        for weight in range(3):
            state(which, weight).start()

    barrier = pltpu.get_barrier_semaphore()
    for offset in (1, -1):
        pl.semaphore_signal(barrier, inc=1, device_id={"dp": at(offset)}, device_id_type=MESH)
    pl.semaphore_wait(barrier, 2)

    sign = (1, -1)
    sends = n - 1

    def distance(k):
        return half - (k + 1) // 2

    def layer(way, k):
        return (way + k) % 2

    def send_sum(way, k, weight):
        if k < 2:
            source = own[weight].at[layer(way, k), pl.ds(block(weight, sign[way] * distance(k)), rows[weight])]
        else:
            source = arrived[weight].at[way, k - 2]
        return pltpu.make_async_remote_copy(
            src_ref=source,
            dst_ref=arrived[weight].at[way, k],
            send_sem=rs_send.at[way, k, weight],
            recv_sem=rs_recv.at[way, k, weight],
            device_id={"dp": at(sign[way])},
            device_id_type=MESH,
        )

    loaded = set()

    def need(weight, offset):
        if (weight, offset % n) not in loaded:
            loaded.add((weight, offset % n))
            load(weight, offset).wait()

    @pl.when(lax.rem(lax.axis_index("rep"), 2) == LATE)
    def _():
        pl.delay(HEAD_START_NS)

    for k in range(2):
        for weight in range(3):
            for way in range(2):
                need(weight, sign[way] * distance(k))
                send_sum(way, k, weight).start()

    def pieces(weight, body, carry=None):
        def step(i, carry):
            r = pl.multiple_of(i * ROWS, ROWS)
            for c in range(0, cols[weight], LANES):
                carry = body(r, pl.ds(c, LANES), carry)
            return carry

        return lax.fori_loop(0, rows[weight] // ROWS, step, carry)

    def add(way, k, weight):
        offset, which = sign[way] * (distance(k) - 1), layer(way, k)
        base = block(weight, offset)

        def body(r, c, carry):
            term = own[weight][which, pl.ds(pl.multiple_of(base + r, ROWS), ROWS), c].astype(F32)
            so_far = arrived[weight][way, k, pl.ds(r, ROWS), c].astype(F32)
            arrived[weight][way, k, pl.ds(r, ROWS), c] = (so_far + term).astype(BF16)
            return carry

        pieces(weight, body, 0)

    for k in range(sends - 2):
        for weight in range(3):
            for way in range(2):
                need(weight, sign[way] * (distance(k) - 1))
                send_sum(way, k, weight).wait_recv()
                add(way, k, weight)
                send_sum(way, k + 2, weight).start()
                send_sum(way, k, weight).wait_send()

    def finish(which, weight, sums):
        base = block(weight, 0)
        first, second = ((way, k) for way in range(2) for k in (sends - 2, sends - 1) if layer(way, k) == which)

        def body(r, c, sums):
            g = own[weight][which, pl.ds(pl.multiple_of(base + r, ROWS), ROWS), c].astype(F32)
            g += arrived[weight][first[0], first[1], pl.ds(r, ROWS), c].astype(F32)
            g += arrived[weight][second[0], second[1], pl.ds(r, ROWS), c].astype(F32)
            g = g.astype(BF16)
            total[weight][which, pl.ds(r, ROWS), c] = g
            g = g.astype(F32)
            g = g * g
            return sums + (g[:8] + g[8:])

        return pieces(weight, body, sums)

    for weight in range(3):
        need(weight, 0)
        for way in range(2):
            send_sum(way, sends - 2, weight).wait_recv()
    sums = jnp.zeros((8, LANES), F32)
    for weight in range(3):
        for way in range(2):
            send_sum(way, sends - 1, weight).wait_recv()
            sums = finish(layer(way, sends - 1), weight, sums)
    sums = sum(sums[:, c : c + 128] for c in range(0, LANES, 128))
    squares[0] = jnp.broadcast_to(jnp.sum(sums, axis=0, keepdims=True), (8, 128))

    def send_squares(offset):
        return pltpu.make_async_remote_copy(
            src_ref=squares.at[0],
            dst_ref=squares.at[offset],
            send_sem=sq_send.at[offset],
            recv_sem=sq_recv.at[offset],
            device_id={"dp": at(offset)},
            device_id_type=MESH,
        )

    far_first = sorted(range(1, n), key=lambda offset: -min(offset, n - offset))
    for offset in far_first:
        send_squares(offset).start()
    for weight in range(3):
        for which in range(3):
            state(which, weight).wait()
        for way in range(2):
            for k in range(sends - 2, sends):
                send_sum(way, k, weight).wait_send()
    everyone = squares[0, :1]
    for offset in reversed(far_first):
        send_squares(offset).wait_recv()
        everyone += squares[offset, :1]
    everyone = jnp.sum(everyone, axis=1, keepdims=True)
    factor = jnp.minimum(1.0, 0.5 * lax.rsqrt(everyone / count + 1e-30))

    def adamw(which, weight):
        def body(r, c, carry):
            part = (which, pl.ds(r, ROWS), c)
            g = total[weight][part].astype(F32) * factor
            w = w_old[weight][part].astype(F32)
            m_new = 0.9 * m[weight][part] + 0.1 * g
            v_new = 0.95 * v[weight][part] + 0.05 * g * g
            m_out[weight][part] = m_new
            v_out[weight][part] = v_new
            step = m_new * lax.rsqrt(v_new + 1e-8) + 0.1 * w
            w_out[weight][part] = (w - 0.02 * step).astype(BF16)
            return carry

        pieces(weight, body, 0)

    for which in range(2):
        for weight in range(3):
            adamw(which, weight)

    for offset in far_first:
        send_squares(offset).wait_send()


def gather(n, count, *refs):
    blocks, whole = refs[:count], refs[count + 1 : 2 * count + 1]
    sends, recvs = refs[2 * count + 1 :]
    half = n // 2
    me = lax.axis_index("dp")
    sign = (1, -1)

    def at(offset):
        return lax.rem(me + offset + n, n)

    barrier = pltpu.get_barrier_semaphore()
    for offset in sign:
        pl.semaphore_signal(barrier, inc=1, device_id={"dp": at(offset)}, device_id_type=MESH)
    pl.semaphore_wait(barrier, 2)

    def copy(way, q, which, weight, behind):
        rows = blocks[weight].shape[1]
        place = whole[weight].at[which, pl.ds(pl.multiple_of(at(-sign[way] * behind) * rows, rows), rows)]
        return pltpu.make_async_remote_copy(
            src_ref=blocks[weight].at[which] if behind == 0 else place,
            dst_ref=place,
            send_sem=sends.at[way, q, which, weight],
            recv_sem=recvs.at[way, q, which, weight],
            device_id={"dp": at(sign[way])},
            device_id_type=MESH,
        )

    def goes(way, q, which):
        return q < half - 1 or (q == half - 1 and which == way)

    for q in range(half + 1):
        for which in range(2):
            for weight in range(count):
                for way in range(2):
                    if q and goes(way, q - 1, which):
                        copy(way, q - 1, which, weight, q).wait_recv()
                    if goes(way, q, which):
                        copy(way, q, which, weight, q).start()
                    if q > 1:
                        copy(way, q - 2, which, weight, q - 2).wait_send()
    for which in range(2):
        for weight in range(count):
            copy(which, half - 1, which, weight, half - 1).wait_send()


def put_state(*refs):
    arrays = len(refs) // 2 - 1
    sem = refs[-1]
    copies = [
        pltpu.make_async_copy(refs[i].at[layer], refs[arrays + i].at[layer], sem.at[i, layer])
        for i in range(arrays)
        for layer in range(2)
    ]
    for copy in copies:
        copy.start()
    for copy in copies:
        copy.wait()


def put_weights(n, count, *refs):
    blocks, whole, out = refs[:count], refs[count : 2 * count], refs[2 * count : 3 * count]
    sem = refs[-1]
    me = lax.axis_index("dp")
    copies = []
    for i in range(count):
        rows = blocks[i].shape[1]
        for layer in range(2):
            for offset in range(n):
                part = pl.ds(pl.multiple_of(lax.rem(me + offset, n) * rows, rows), rows)
                source = blocks[i].at[layer] if offset == 0 else whole[i].at[layer, part]
                copies.append(pltpu.make_async_copy(source, out[i].at[layer, part], sem.at[i, layer, offset]))
    for copy in copies:
        copy.start()
    for copy in copies:
        copy.wait()


def solution(mesh):
    n = mesh.shape["dp"]

    def step(*arrays):
        terms, weights, m, v = (arrays[i : i + 3] for i in (0, 3, 6, 9))
        terms = tuple(t[0] for t in terms)
        half = n // 2
        shapes = [one.shape for one in m]
        dma = pltpu.SemaphoreType.DMA
        scratch = [pltpu.VMEM(t.shape, t.dtype) for t in terms]
        scratch += [pltpu.VMEM((2, n - 1, *s[1:]), BF16) for s in shapes]
        scratch += [pltpu.VMEM(s, BF16) for _ in range(2) for s in shapes]
        scratch += [pltpu.VMEM(s, F32) for _ in range(2) for s in shapes]
        scratch += [
            pltpu.VMEM((n, 8, 128), F32),
            dma((3, n)),
            dma((3, 3)),
            dma((2, n - 1, 3)),
            dma((2, n - 1, 3)),
            dma((n,)),
            dma((n,)),
        ]
        hbm, vmem, anywhere = (pl.BlockSpec(memory_space=space) for space in (pltpu.HBM, pltpu.VMEM, pl.ANY))

        def in_vmem(arrays):
            return [pltpu.with_memory_space_constraint(one, pltpu.VMEM) for one in arrays]

        def plain(body, arrays, out, sems):
            token = jax.ShapeDtypeStruct((8, 128), F32)
            *out, token = pl.pallas_call(
                body,
                out_shape=[*(jax.ShapeDtypeStruct(one.shape, one.dtype) for one in out), token],
                in_specs=[vmem] * len(arrays),
                out_specs=[anywhere] * (len(out) + 1),
                scratch_shapes=[dma(sems)],
                compiler_params=pltpu.CompilerParams(vmem_limit_bytes=2**20, has_side_effects=True),
            )(*in_vmem(arrays))
            return out, token

        def gathered(blocks, shapes, token, collective_id):
            count = len(blocks)
            whole = pl.pallas_call(
                functools.partial(gather, n, count),
                out_shape=[pltpu.VMEM(one.shape, one.dtype) for one in shapes],
                in_specs=[vmem] * count + [anywhere],
                out_specs=[vmem] * count,
                scratch_shapes=[dma((2, half, 2, count))] * 2,
                compiler_params=pltpu.CompilerParams(collective_id=collective_id, has_side_effects=True, vmem_limit_bytes=2**20),
            )(*in_vmem(blocks), token)
            return plain(functools.partial(put_weights, n, count), (*blocks, *whole), shapes, (count, 2, n))

        in_hbm = [pltpu.with_memory_space_constraint(one, pltpu.HBM) for one in (*terms, *weights, *m, *v)]
        results = [(s, BF16) for s in shapes] + [(s, F32) for s in shapes] * 2
        new = pl.pallas_call(
            functools.partial(reduce_and_step, n),
            out_shape=[pltpu.VMEM(*one) for one in results],
            in_specs=[hbm] * len(in_hbm),
            out_specs=[vmem] * len(results),
            scratch_shapes=scratch,
            compiler_params=pltpu.CompilerParams(collective_id=0, has_side_effects=True, vmem_limit_bytes=28 * 2**20),
        )(*in_hbm)
        blocks = new[:3]
        state, token = plain(put_state, new[3:], new[3:], (6, 2))
        whole, _ = gathered(blocks, weights, token, 1)
        return (*whole, *state)

    all_of, cut = P(None, None, None), P(None, "dp", None)
    return jax.shard_map(
        step,
        mesh=mesh,
        in_specs=(P(("rep", "dp"), None, None, None),) * 3 + (all_of,) * 3 + (cut,) * 6,
        out_specs=(P("rep", None, None),) * 3 + (P("rep", "dp", None),) * 6,
        check_vma=False,
    )
```

```python
import functools

import jax
import jax.numpy as jnp
from jax import lax
from jax.experimental import pallas as pl
from jax.experimental.pallas import tpu as pltpu
from jax.sharding import PartitionSpec as P

MESH = pl.DeviceIdType.MESH
F32, BF16 = jnp.float32, jnp.bfloat16
ROWS, LANES = 16, 256

LATE, HEAD_START_NS = 0, 12000
NEAR = 2


def pieces(rows, cols, body, carry):
    def step(i, carry):
        r = pl.multiple_of(i * ROWS, ROWS)
        for c in range(0, cols, LANES):
            carry = body(r, pl.ds(c, LANES), carry)
        return carry

    return lax.fori_loop(0, rows // ROWS, step, carry)


def reduce_and_norm(n, *refs):
    terms, weights, m_in, v_in = (refs[i : i + 3] for i in (0, 3, 6, 9))
    total, w_old, m, v = (refs[i : i + 3] for i in (12, 15, 18, 21))
    factor, *refs = refs[24:]
    own, arrived = refs[:3], refs[3:6]
    squares, load_sem, state_sem, rs_send, rs_recv, sq_send, sq_recv = refs[6:]

    half = n // 2
    me = lax.axis_index("dp")
    rows = [ref.shape[1] for ref in m_in]
    cols = [ref.shape[2] for ref in m_in]
    count = n * sum(2 * r * c for r, c in zip(rows, cols, strict=True))

    def at(offset):
        return lax.rem(me + offset + n, n)

    def block(weight, offset):
        return pl.multiple_of(at(offset) * rows[weight], rows[weight])

    def load(weight, offset):
        part = pl.ds(block(weight, offset), rows[weight])
        return pltpu.make_async_copy(terms[weight].at[:, part], own[weight].at[:, part], load_sem.at[weight, offset % n])

    order = [half]
    for distance in range(half - 1, 0, -1):
        order += [distance, -distance]
    order += [0]
    for offset in order:
        for weight in range(3):
            load(weight, offset).start()

    def state(which, weight):
        if which == 0:
            return pltpu.make_async_copy(weights[weight].at[:, pl.ds(block(weight, 0), rows[weight])], w_old[weight], state_sem.at[0, weight])
        source, target = ((m_in, m), (v_in, v))[which - 1]
        return pltpu.make_async_copy(source[weight], target[weight], state_sem.at[which, weight])

    for which in range(3):
        for weight in range(3):
            state(which, weight).start()

    barrier = pltpu.get_barrier_semaphore()
    for offset in (1, -1):
        pl.semaphore_signal(barrier, inc=1, device_id={"dp": at(offset)}, device_id_type=MESH)
    pl.semaphore_wait(barrier, 2)

    sign = (1, -1)
    sends = n - 1

    def distance(k):
        return half - (k + 1) // 2

    def layer(way, k):
        return (way + k) % 2

    def send_sum(way, k, weight):
        if k < 2:
            source = own[weight].at[layer(way, k), pl.ds(block(weight, sign[way] * distance(k)), rows[weight])]
        else:
            source = arrived[weight].at[way, k - 2]
        return pltpu.make_async_remote_copy(
            src_ref=source,
            dst_ref=arrived[weight].at[way, k],
            send_sem=rs_send.at[way, k, weight],
            recv_sem=rs_recv.at[way, k, weight],
            device_id={"dp": at(sign[way])},
            device_id_type=MESH,
        )

    loaded = set()

    def need(weight, offset):
        if (weight, offset % n) not in loaded:
            loaded.add((weight, offset % n))
            load(weight, offset).wait()

    @pl.when(lax.rem(lax.axis_index("rep"), 2) == LATE)
    def _():
        pl.delay(HEAD_START_NS)

    for k in range(2):
        for weight in range(3):
            for way in range(2):
                need(weight, sign[way] * distance(k))
                send_sum(way, k, weight).start()

    def add(way, k, weight):
        offset, which = sign[way] * (distance(k) - 1), layer(way, k)
        base = block(weight, offset)

        def body(r, c, carry):
            term = own[weight][which, pl.ds(pl.multiple_of(base + r, ROWS), ROWS), c].astype(F32)
            so_far = arrived[weight][way, k, pl.ds(r, ROWS), c].astype(F32)
            arrived[weight][way, k, pl.ds(r, ROWS), c] = (so_far + term).astype(BF16)
            return carry

        pieces(rows[weight], cols[weight], body, 0)

    for k in range(sends - 2):
        for weight in range(3):
            for way in range(2):
                need(weight, sign[way] * (distance(k) - 1))
                send_sum(way, k, weight).wait_recv()
                add(way, k, weight)
                send_sum(way, k + 2, weight).start()
                send_sum(way, k, weight).wait_send()

    def finish(which, weight, sums):
        base = block(weight, 0)
        first, second = ((way, k) for way in range(2) for k in (sends - 2, sends - 1) if layer(way, k) == which)

        def body(r, c, sums):
            g = own[weight][which, pl.ds(pl.multiple_of(base + r, ROWS), ROWS), c].astype(F32)
            g += arrived[weight][first[0], first[1], pl.ds(r, ROWS), c].astype(F32)
            g += arrived[weight][second[0], second[1], pl.ds(r, ROWS), c].astype(F32)
            g = g.astype(BF16)
            total[weight][which, pl.ds(r, ROWS), c] = g
            g = g.astype(F32)
            g = g * g
            return sums + (g[:8] + g[8:])

        return pieces(rows[weight], cols[weight], body, sums)

    for weight in range(3):
        need(weight, 0)
        for way in range(2):
            send_sum(way, sends - 2, weight).wait_recv()
    sums = jnp.zeros((8, LANES), F32)
    for weight in range(3):
        for way in range(2):
            send_sum(way, sends - 1, weight).wait_recv()
            sums = finish(layer(way, sends - 1), weight, sums)
    sums = sum(sums[:, c : c + 128] for c in range(0, LANES, 128))
    squares[0] = jnp.broadcast_to(jnp.sum(sums, axis=0, keepdims=True), (8, 128))

    def send_squares(offset):
        return pltpu.make_async_remote_copy(
            src_ref=squares.at[0],
            dst_ref=squares.at[offset],
            send_sem=sq_send.at[offset],
            recv_sem=sq_recv.at[offset],
            device_id={"dp": at(offset)},
            device_id_type=MESH,
        )

    far_first = sorted(range(1, n), key=lambda offset: -min(offset, n - offset))
    for offset in far_first:
        send_squares(offset).start()
    for weight in range(3):
        for which in range(3):
            state(which, weight).wait()
        for way in range(2):
            for k in range(sends - 2, sends):
                send_sum(way, k, weight).wait_send()
    everyone = squares[0, :1]
    for offset in reversed(far_first):
        send_squares(offset).wait_recv()
        everyone += squares[offset, :1]
    everyone = jnp.sum(everyone, axis=1, keepdims=True)
    factor[...] = jnp.broadcast_to(jnp.minimum(1.0, 0.5 * lax.rsqrt(everyone / count + 1e-30)), factor.shape)

    for offset in far_first:
        send_squares(offset).wait_send()


def adamw(*refs):
    total, w_old, m, v = (refs[i : i + 3] for i in (0, 3, 6, 9))
    factor = refs[12][:1, :1]
    w_new, m_out, v_out = (refs[i : i + 3] for i in (13, 16, 19))
    m_new, v_new = refs[23:26], refs[26:29]
    sem = refs[29]
    copies = []
    for which in range(2):
        for weight in range(3):

            def body(r, c, carry, which=which, weight=weight):
                part = (which, pl.ds(r, ROWS), c)
                g = total[weight][part].astype(F32) * factor
                w = w_old[weight][part].astype(F32)
                moment = 0.9 * m[weight][part] + 0.1 * g
                second = 0.95 * v[weight][part] + 0.05 * g * g
                m_new[weight][part] = moment
                v_new[weight][part] = second
                step = moment * lax.rsqrt(second + 1e-8) + 0.1 * w
                w_new[weight][part] = (w - 0.02 * step).astype(BF16)
                return carry

            pieces(m[weight].shape[1], m[weight].shape[2], body, 0)
            for i, (source, target) in enumerate(((m_new, m_out), (v_new, v_out))):
                copy = pltpu.make_async_copy(source[weight].at[which], target[weight].at[which], sem.at[i, which, weight])
                copy.start()
                copies.append(copy)
    for copy in copies:
        copy.wait()


def gather(n, first, last, *refs):
    count = (len(refs) - 3) // 2
    before, whole = refs[:count], refs[count + 1 : 2 * count + 1]
    sends, recvs = refs[2 * count + 1 :]
    half = n // 2
    me = lax.axis_index("dp")
    sign = (1, -1)

    def at(offset):
        return lax.rem(me + offset + n, n)

    barrier = pltpu.get_barrier_semaphore()
    for offset in sign:
        pl.semaphore_signal(barrier, inc=1, device_id={"dp": at(offset)}, device_id_type=MESH)
    pl.semaphore_wait(barrier, 2)

    def copy(way, q, which, weight, behind):
        rows = whole[weight].shape[1] // n
        part = (which, pl.ds(pl.multiple_of(at(-sign[way] * behind) * rows, rows), rows))
        if behind == 0:
            source = before[weight].at[which]
        else:
            source = (before if behind == first else whole)[weight].at[part]
        return pltpu.make_async_remote_copy(
            src_ref=source,
            dst_ref=whole[weight].at[part],
            send_sem=sends.at[way, q - first, which, weight],
            recv_sem=recvs.at[way, q - first, which, weight],
            device_id={"dp": at(sign[way])},
            device_id_type=MESH,
        )

    def goes(way, q, which):
        return q < half - 1 or which == way

    def keep(which, weight):
        rows, cols = before[weight].shape[1:]

        def body(r, c, carry):
            whole[weight][which, pl.ds(pl.multiple_of(me * rows + r, ROWS), ROWS), c] = before[weight][which, pl.ds(r, ROWS), c]
            return carry

        pieces(rows, cols, body, 0)

    each = [(which, weight) for which in range(2) for weight in range(count)]
    for q in range(first, last + 1):
        for which, weight in each:
            for way in range(2):
                if q > first and goes(way, q - 1, which):
                    copy(way, q - 1, which, weight, q).wait_recv()
                if q < last and goes(way, q, which):
                    copy(way, q, which, weight, q).start()
                if q > first + 1:
                    copy(way, q - 2, which, weight, q - 2).wait_send()
        if q == 0:
            for which, weight in each:
                keep(which, weight)
    for which, weight in each:
        for way in range(2):
            if goes(way, last - 1, which):
                copy(way, last - 1, which, weight, last - 1).wait_send()


def put_out(n, offsets, *refs):
    whole, out, sem = refs[:3], refs[-5:-2], refs[-1]
    me = lax.axis_index("dp")
    copies = []
    for i in range(3):
        rows = whole[i].shape[1] // n
        for j, offset in enumerate(offsets):
            part = pl.ds(pl.multiple_of(lax.rem(me + offset, n) * rows, rows), rows)
            copies.append(pltpu.make_async_copy(whole[i].at[:, part], out[i].at[:, part], sem.at[i, j]))
    for copy in copies:
        copy.start()
    for copy in copies:
        copy.wait()


def solution(mesh):
    n = mesh.shape["dp"]

    def step(*arrays):
        terms, weights, m, v = (arrays[i : i + 3] for i in (0, 3, 6, 9))
        terms = tuple(t[0] for t in terms)
        half = n // 2
        shapes = [one.shape for one in m]
        dma = pltpu.SemaphoreType.DMA
        scratch = [pltpu.VMEM(t.shape, t.dtype) for t in terms]
        scratch += [pltpu.VMEM((2, n - 1, *s[1:]), BF16) for s in shapes]
        scratch += [
            pltpu.VMEM((n, 8, 128), F32),
            dma((3, n)),
            dma((3, 3)),
            dma((2, n - 1, 3)),
            dma((2, n - 1, 3)),
            dma((n,)),
            dma((n,)),
        ]
        hbm, vmem, anywhere = (pl.BlockSpec(memory_space=space) for space in (pltpu.HBM, pltpu.VMEM, pl.ANY))

        def in_vmem(arrays):
            return [pltpu.with_memory_space_constraint(one, pltpu.VMEM) for one in arrays]

        token = jax.ShapeDtypeStruct((8, 128), F32)
        limit = pltpu.CompilerParams(vmem_limit_bytes=2**20, has_side_effects=True)

        def gathered(before, first, last, after, collective_id):
            return pl.pallas_call(
                functools.partial(gather, n, first, last),
                out_shape=[pltpu.VMEM(one.shape, one.dtype) for one in weights],
                in_specs=[vmem] * 3 + [anywhere],
                out_specs=[vmem] * 3,
                scratch_shapes=[dma((2, last - first, 2, 3))] * 2,
                compiler_params=pltpu.CompilerParams(collective_id=collective_id, has_side_effects=True, vmem_limit_bytes=2**20),
            )(*in_vmem(before), after)

        def written(whole, offsets, so_far):
            *out, after = pl.pallas_call(
                functools.partial(put_out, n, offsets),
                out_shape=[*(jax.ShapeDtypeStruct(one.shape, one.dtype) for one in weights), token],
                in_specs=[vmem] * 3 + [anywhere] * len(so_far),
                out_specs=[anywhere] * 4,
                scratch_shapes=[dma((3, len(offsets)))],
                input_output_aliases={3 + i: i for i in range(len(so_far))},
                compiler_params=limit,
            )(*in_vmem(whole), *so_far)
            return out, after

        in_hbm = [pltpu.with_memory_space_constraint(one, pltpu.HBM) for one in (*terms, *weights, *m, *v)]
        results = [(s, BF16) for s in shapes] * 2 + [(s, F32) for s in shapes] * 2 + [((8, 128), F32)]
        summed = pl.pallas_call(
            functools.partial(reduce_and_norm, n),
            out_shape=[pltpu.VMEM(*one) for one in results],
            in_specs=[hbm] * len(in_hbm),
            out_specs=[vmem] * len(results),
            scratch_shapes=scratch,
            compiler_params=pltpu.CompilerParams(collective_id=0, has_side_effects=True, vmem_limit_bytes=20 * 2**20),
        )(*in_hbm)
        *new, after = pl.pallas_call(
            adamw,
            out_shape=[pltpu.VMEM(s, BF16) for s in shapes] + [jax.ShapeDtypeStruct(s, F32) for s in shapes] * 2 + [token],
            in_specs=[vmem] * len(summed),
            out_specs=[vmem] * 3 + [anywhere] * 7,
            scratch_shapes=[pltpu.VMEM(s, F32) for s in shapes] * 2 + [dma((2, 2, 3))],
            compiler_params=pltpu.CompilerParams(vmem_limit_bytes=6 * 2**20, has_side_effects=True),
        )(*in_vmem(summed))
        blocks, state = new[:3], new[3:]
        near = gathered(blocks, 0, NEAR, after, 1)
        out, after = written(near, [offset % n for offset in range(-NEAR, NEAR + 1)], ())
        far = gathered(near, NEAR, half, after, 2)
        out, _ = written(far, range(NEAR + 1, n - NEAR), out)
        return (*out, *state)

    all_of, cut = P(None, None, None), P(None, "dp", None)
    return jax.shard_map(
        step,
        mesh=mesh,
        in_specs=(P(("rep", "dp"), None, None, None),) * 3 + (all_of,) * 3 + (cut,) * 6,
        out_specs=(P("rep", None, None),) * 3 + (P("rep", "dp", None),) * 6,
        check_vma=False,
    )
```

```python
import functools

import jax
import jax.numpy as jnp
from jax import lax
from jax.experimental import pallas as pl
from jax.experimental.pallas import tpu as pltpu
from jax.sharding import PartitionSpec as P

MESH = pl.DeviceIdType.MESH
F32, BF16 = jnp.float32, jnp.bfloat16
ROWS, LANES = 16, 256

LATE, HEAD_START_NS = 0, 11500
NEAR = 2


def pieces(rows, cols, body, carry):
    def step(i, carry):
        r = pl.multiple_of(i * ROWS, ROWS)
        for c in range(0, cols, LANES):
            carry = body(r, pl.ds(c, LANES), carry)
        return carry

    return lax.fori_loop(0, rows // ROWS, step, carry)


def reduce_and_norm(n, *refs):
    terms, weights, m_in, v_in = (refs[i : i + 3] for i in (0, 3, 6, 9))
    total, w_old, m, v = (refs[i : i + 3] for i in (12, 15, 18, 21))
    factor, *refs = refs[24:]
    own, arrived = refs[:3], refs[3:6]
    squares, load_sem, state_sem, rs_send, rs_recv, sq_send, sq_recv = refs[6:]

    half = n // 2
    me = lax.axis_index("dp")
    rows = [ref.shape[1] for ref in m_in]
    cols = [ref.shape[2] for ref in m_in]
    count = n * sum(2 * r * c for r, c in zip(rows, cols, strict=True))

    def at(offset):
        return lax.rem(me + offset + n, n)

    def block(weight, offset):
        return pl.multiple_of(at(offset) * rows[weight], rows[weight])

    def load(weight, offset):
        part = pl.ds(block(weight, offset), rows[weight])
        return pltpu.make_async_copy(terms[weight].at[:, part], own[weight].at[:, part], load_sem.at[weight, offset % n])

    order = [half]
    for distance in range(half - 1, 0, -1):
        order += [distance, -distance]
    order += [0]
    for offset in order:
        for weight in range(3):
            load(weight, offset).start()

    def state(which, weight):
        if which == 0:
            return pltpu.make_async_copy(weights[weight].at[:, pl.ds(block(weight, 0), rows[weight])], w_old[weight], state_sem.at[0, weight])
        source, target = ((m_in, m), (v_in, v))[which - 1]
        return pltpu.make_async_copy(source[weight], target[weight], state_sem.at[which, weight])

    for which in range(3):
        for weight in range(3):
            state(which, weight).start()

    barrier = pltpu.get_barrier_semaphore()
    for offset in (1, -1):
        pl.semaphore_signal(barrier, inc=1, device_id={"dp": at(offset)}, device_id_type=MESH)
    pl.semaphore_wait(barrier, 2)

    sign = (1, -1)
    sends = n - 1

    def distance(k):
        return half - (k + 1) // 2

    def layer(way, k):
        return (way + k) % 2

    def send_sum(way, k, weight):
        if k < 2:
            source = own[weight].at[layer(way, k), pl.ds(block(weight, sign[way] * distance(k)), rows[weight])]
        else:
            source = arrived[weight].at[way, k - 2]
        return pltpu.make_async_remote_copy(
            src_ref=source,
            dst_ref=arrived[weight].at[way, k],
            send_sem=rs_send.at[way, k, weight],
            recv_sem=rs_recv.at[way, k, weight],
            device_id={"dp": at(sign[way])},
            device_id_type=MESH,
        )

    loaded = set()

    def need(weight, offset):
        if (weight, offset % n) not in loaded:
            loaded.add((weight, offset % n))
            load(weight, offset).wait()

    @pl.when(lax.rem(lax.axis_index("rep"), 2) == LATE)
    def _():
        pl.delay(HEAD_START_NS)

    for k in range(2):
        for weight in range(3):
            for way in range(2):
                need(weight, sign[way] * distance(k))
                send_sum(way, k, weight).start()

    def add(way, k, weight):
        offset, which = sign[way] * (distance(k) - 1), layer(way, k)
        base = block(weight, offset)

        def body(r, c, carry):
            term = own[weight][which, pl.ds(pl.multiple_of(base + r, ROWS), ROWS), c].astype(F32)
            so_far = arrived[weight][way, k, pl.ds(r, ROWS), c].astype(F32)
            arrived[weight][way, k, pl.ds(r, ROWS), c] = (so_far + term).astype(BF16)
            return carry

        pieces(rows[weight], cols[weight], body, 0)

    for k in range(sends - 2):
        for weight in range(3):
            for way in range(2):
                need(weight, sign[way] * (distance(k) - 1))
                send_sum(way, k, weight).wait_recv()
                add(way, k, weight)
            for way in range(2):
                send_sum(way, k + 2, weight).start()
            for way in range(2):
                send_sum(way, k, weight).wait_send()

    def finish(which, weight, sums):
        base = block(weight, 0)
        first, second = ((way, k) for way in range(2) for k in (sends - 2, sends - 1) if layer(way, k) == which)

        def body(r, c, sums):
            g = own[weight][which, pl.ds(pl.multiple_of(base + r, ROWS), ROWS), c].astype(F32)
            g += arrived[weight][first[0], first[1], pl.ds(r, ROWS), c].astype(F32)
            g += arrived[weight][second[0], second[1], pl.ds(r, ROWS), c].astype(F32)
            g = g.astype(BF16)
            total[weight][which, pl.ds(r, ROWS), c] = g
            g = g.astype(F32)
            g = g * g
            return sums + (g[:8] + g[8:])

        return pieces(rows[weight], cols[weight], body, sums)

    for weight in range(3):
        need(weight, 0)
        for way in range(2):
            send_sum(way, sends - 2, weight).wait_recv()
    sums = jnp.zeros((8, LANES), F32)
    for weight in range(3):
        for way in range(2):
            send_sum(way, sends - 1, weight).wait_recv()
            sums = finish(layer(way, sends - 1), weight, sums)
    sums = sum(sums[:, c : c + 128] for c in range(0, LANES, 128))
    squares[0] = jnp.broadcast_to(jnp.sum(sums, axis=0, keepdims=True), (8, 128))

    def send_squares(offset):
        return pltpu.make_async_remote_copy(
            src_ref=squares.at[0],
            dst_ref=squares.at[offset],
            send_sem=sq_send.at[offset],
            recv_sem=sq_recv.at[offset],
            device_id={"dp": at(offset)},
            device_id_type=MESH,
        )

    far_first = sorted(range(1, n), key=lambda offset: -min(offset, n - offset))
    for weight in range(3):
        for which in range(3):
            state(which, weight).wait()
    for offset in far_first:
        send_squares(offset).start()
    for weight in range(3):
        for way in range(2):
            for k in range(sends - 2, sends):
                send_sum(way, k, weight).wait_send()
    everyone = squares[0, :1]
    for offset in reversed(far_first):
        send_squares(offset).wait_recv()
        everyone += squares[offset, :1]
    everyone = jnp.sum(everyone, axis=1, keepdims=True)
    factor[...] = jnp.broadcast_to(jnp.minimum(1.0, 0.5 * lax.rsqrt(everyone / count + 1e-30)), factor.shape)

    for offset in far_first:
        send_squares(offset).wait_send()


def adamw(*refs):
    total, w_old, m, v = (refs[i : i + 3] for i in (0, 3, 6, 9))
    factor = refs[12][:1, :1]
    w_new, m_out, v_out = (refs[i : i + 3] for i in (13, 16, 19))
    m_new, v_new = refs[23:26], refs[26:29]
    sem = refs[29]
    copies = []
    for which in range(2):
        for weight in range(3):

            def body(r, c, carry, which=which, weight=weight):
                part = (which, pl.ds(r, ROWS), c)
                g = total[weight][part].astype(F32) * factor
                w = w_old[weight][part].astype(F32)
                moment = 0.9 * m[weight][part] + 0.1 * g
                second = 0.95 * v[weight][part] + 0.05 * g * g
                m_new[weight][part] = moment
                v_new[weight][part] = second
                step = moment * lax.rsqrt(second + 1e-8) + 0.1 * w
                w_new[weight][part] = (w - 0.02 * step).astype(BF16)
                return carry

            pieces(m[weight].shape[1], m[weight].shape[2], body, 0)
            for i, (source, target) in enumerate(((m_new, m_out), (v_new, v_out))):
                copy = pltpu.make_async_copy(source[weight].at[which], target[weight].at[which], sem.at[i, which, weight])
                copy.start()
                copies.append(copy)
    for copy in copies:
        copy.wait()


def gather(n, first, last, *refs):
    count = (len(refs) - 3) // 2
    before, whole = refs[:count], refs[count + 1 : 2 * count + 1]
    sends, recvs = refs[2 * count + 1 :]
    half = n // 2
    me = lax.axis_index("dp")
    sign = (1, -1)

    def at(offset):
        return lax.rem(me + offset + n, n)

    barrier = pltpu.get_barrier_semaphore()
    for offset in sign:
        pl.semaphore_signal(barrier, inc=1, device_id={"dp": at(offset)}, device_id_type=MESH)
    pl.semaphore_wait(barrier, 2)

    def copy(way, q, which, weight, behind):
        rows = whole[weight].shape[1] // n
        part = (which, pl.ds(pl.multiple_of(at(-sign[way] * behind) * rows, rows), rows))
        if behind == 0:
            source = before[weight].at[which]
        else:
            source = (before if behind == first else whole)[weight].at[part]
        return pltpu.make_async_remote_copy(
            src_ref=source,
            dst_ref=whole[weight].at[part],
            send_sem=sends.at[way, q - first, which, weight],
            recv_sem=recvs.at[way, q - first, which, weight],
            device_id={"dp": at(sign[way])},
            device_id_type=MESH,
        )

    def goes(way, q, which):
        return q < half - 1 or which == way

    def keep(which, weight):
        rows, cols = before[weight].shape[1:]

        def body(r, c, carry):
            whole[weight][which, pl.ds(pl.multiple_of(me * rows + r, ROWS), ROWS), c] = before[weight][which, pl.ds(r, ROWS), c]
            return carry

        pieces(rows, cols, body, 0)

    each = [(which, weight) for which in range(2) for weight in range(count)]
    for q in range(first, last + 1):
        for which, weight in each:
            for way in range(2):
                if q > first and goes(way, q - 1, which):
                    copy(way, q - 1, which, weight, q).wait_recv()
                if q < last and goes(way, q, which):
                    copy(way, q, which, weight, q).start()
                if q > first + 1:
                    copy(way, q - 2, which, weight, q - 2).wait_send()
        if q == 0:
            for which, weight in each:
                keep(which, weight)
    for which, weight in each:
        for way in range(2):
            if goes(way, last - 1, which):
                copy(way, last - 1, which, weight, last - 1).wait_send()


def put_out(n, offsets, *refs):
    whole, out, sem = refs[:3], refs[-5:-2], refs[-1]
    me = lax.axis_index("dp")
    copies = []
    for i in range(3):
        rows = whole[i].shape[1] // n
        for j, offset in enumerate(offsets):
            part = pl.ds(pl.multiple_of(lax.rem(me + offset, n) * rows, rows), rows)
            copies.append(pltpu.make_async_copy(whole[i].at[:, part], out[i].at[:, part], sem.at[i, j]))
    for copy in copies:
        copy.start()
    for copy in copies:
        copy.wait()


def solution(mesh):
    n = mesh.shape["dp"]

    def step(*arrays):
        terms, weights, m, v = (arrays[i : i + 3] for i in (0, 3, 6, 9))
        terms = tuple(t[0] for t in terms)
        half = n // 2
        shapes = [one.shape for one in m]
        dma = pltpu.SemaphoreType.DMA
        scratch = [pltpu.VMEM(t.shape, t.dtype) for t in terms]
        scratch += [pltpu.VMEM((2, n - 1, *s[1:]), BF16) for s in shapes]
        scratch += [
            pltpu.VMEM((n, 8, 128), F32),
            dma((3, n)),
            dma((3, 3)),
            dma((2, n - 1, 3)),
            dma((2, n - 1, 3)),
            dma((n,)),
            dma((n,)),
        ]
        hbm, vmem, anywhere = (pl.BlockSpec(memory_space=space) for space in (pltpu.HBM, pltpu.VMEM, pl.ANY))

        def in_vmem(arrays):
            return [pltpu.with_memory_space_constraint(one, pltpu.VMEM) for one in arrays]

        token = jax.ShapeDtypeStruct((8, 128), F32)
        limit = pltpu.CompilerParams(vmem_limit_bytes=2**20, has_side_effects=True)

        def gathered(before, first, last, after, collective_id):
            return pl.pallas_call(
                functools.partial(gather, n, first, last),
                out_shape=[pltpu.VMEM(one.shape, one.dtype) for one in weights],
                in_specs=[vmem] * 3 + [anywhere],
                out_specs=[vmem] * 3,
                scratch_shapes=[dma((2, last - first, 2, 3))] * 2,
                compiler_params=pltpu.CompilerParams(collective_id=collective_id, has_side_effects=True, vmem_limit_bytes=2**20),
            )(*in_vmem(before), after)

        def written(whole, offsets, so_far):
            *out, after = pl.pallas_call(
                functools.partial(put_out, n, offsets),
                out_shape=[*(jax.ShapeDtypeStruct(one.shape, one.dtype) for one in weights), token],
                in_specs=[vmem] * 3 + [anywhere] * len(so_far),
                out_specs=[anywhere] * 4,
                scratch_shapes=[dma((3, len(offsets)))],
                input_output_aliases={3 + i: i for i in range(len(so_far))},
                compiler_params=limit,
            )(*in_vmem(whole), *so_far)
            return out, after

        in_hbm = [pltpu.with_memory_space_constraint(one, pltpu.HBM) for one in (*terms, *weights, *m, *v)]
        results = [(s, BF16) for s in shapes] * 2 + [(s, F32) for s in shapes] * 2 + [((8, 128), F32)]
        summed = pl.pallas_call(
            functools.partial(reduce_and_norm, n),
            out_shape=[pltpu.VMEM(*one) for one in results],
            in_specs=[hbm] * len(in_hbm),
            out_specs=[vmem] * len(results),
            scratch_shapes=scratch,
            compiler_params=pltpu.CompilerParams(collective_id=0, has_side_effects=True, vmem_limit_bytes=20 * 2**20),
        )(*in_hbm)
        *new, after = pl.pallas_call(
            adamw,
            out_shape=[pltpu.VMEM(s, BF16) for s in shapes] + [jax.ShapeDtypeStruct(s, F32) for s in shapes] * 2 + [token],
            in_specs=[vmem] * len(summed),
            out_specs=[vmem] * 3 + [anywhere] * 7,
            scratch_shapes=[pltpu.VMEM(s, F32) for s in shapes] * 2 + [dma((2, 2, 3))],
            compiler_params=pltpu.CompilerParams(vmem_limit_bytes=6 * 2**20, has_side_effects=True),
        )(*in_vmem(summed))
        blocks, state = new[:3], new[3:]
        near = gathered(blocks, 0, NEAR, after, 1)
        out, after = written(near, [offset % n for offset in range(-NEAR, NEAR + 1)], ())
        far = gathered(near, NEAR, half, after, 2)
        out, _ = written(far, range(NEAR + 1, n - NEAR), out)
        return (*out, *state)

    all_of, cut = P(None, None, None), P(None, "dp", None)
    return jax.shard_map(
        step,
        mesh=mesh,
        in_specs=(P(("rep", "dp"), None, None, None),) * 3 + (all_of,) * 3 + (cut,) * 6,
        out_specs=(P("rep", None, None),) * 3 + (P("rep", "dp", None),) * 6,
        check_vma=False,
    )
```

```python
import functools

import jax
import jax.numpy as jnp
from jax import lax
from jax.experimental import pallas as pl
from jax.experimental.pallas import tpu as pltpu
from jax.sharding import PartitionSpec as P

MESH = pl.DeviceIdType.MESH
F32, BF16 = jnp.float32, jnp.bfloat16
ROWS, LANES = 16, 256

LATE, HEAD_START_NS = 0, 11500
NEAR = 2


def pieces(rows, cols, body, carry):
    def step(i, carry):
        r = pl.multiple_of(i * ROWS, ROWS)
        for c in range(0, cols, LANES):
            carry = body(r, pl.ds(c, LANES), carry)
        return carry

    return lax.fori_loop(0, rows // ROWS, step, carry)


def reduce_and_norm(n, *refs):
    terms, weights, m_in, v_in = (refs[i : i + 3] for i in (0, 3, 6, 9))
    total, w_old, m, v = (refs[i : i + 3] for i in (12, 15, 18, 21))
    factor, *refs = refs[24:]
    own, arrived = refs[:3], refs[3:6]
    squares, load_sem, state_sem, rs_send, rs_recv, sq_send, sq_recv = refs[6:]

    half = n // 2
    me = lax.axis_index("dp")
    rows = [ref.shape[1] for ref in m_in]
    cols = [ref.shape[2] for ref in m_in]
    count = n * sum(2 * r * c for r, c in zip(rows, cols, strict=True))

    def at(offset):
        return lax.rem(me + offset + n, n)

    def block(weight, offset):
        return pl.multiple_of(at(offset) * rows[weight], rows[weight])

    def load(weight, offset):
        part = pl.ds(block(weight, offset), rows[weight])
        return pltpu.make_async_copy(terms[weight].at[:, part], own[weight].at[:, part], load_sem.at[weight, offset % n])

    order = [half]
    for distance in range(half - 1, 0, -1):
        order += [distance, -distance]
    order += [0]
    for offset in order:
        for weight in range(3):
            load(weight, offset).start()

    def state(which, weight):
        if which == 0:
            return pltpu.make_async_copy(weights[weight].at[:, pl.ds(block(weight, 0), rows[weight])], w_old[weight], state_sem.at[0, weight])
        source, target = ((m_in, m), (v_in, v))[which - 1]
        return pltpu.make_async_copy(source[weight], target[weight], state_sem.at[which, weight])

    for which in range(3):
        for weight in range(3):
            state(which, weight).start()

    barrier = pltpu.get_barrier_semaphore()
    for offset in (1, -1):
        pl.semaphore_signal(barrier, inc=1, device_id={"dp": at(offset)}, device_id_type=MESH)
    pl.semaphore_wait(barrier, 2)

    sign = (1, -1)
    sends = n - 1

    def distance(k):
        return half - (k + 1) // 2

    def layer(way, k):
        return (way + k) % 2

    def send_sum(way, k, weight):
        if k < 2:
            source = own[weight].at[layer(way, k), pl.ds(block(weight, sign[way] * distance(k)), rows[weight])]
        else:
            source = arrived[weight].at[way, k - 2]
        return pltpu.make_async_remote_copy(
            src_ref=source,
            dst_ref=arrived[weight].at[way, k],
            send_sem=rs_send.at[way, k, weight],
            recv_sem=rs_recv.at[way, k, weight],
            device_id={"dp": at(sign[way])},
            device_id_type=MESH,
        )

    loaded = set()

    def need(weight, offset):
        if (weight, offset % n) not in loaded:
            loaded.add((weight, offset % n))
            load(weight, offset).wait()

    @pl.when(lax.rem(lax.axis_index("rep"), 2) == LATE)
    def _():
        pl.delay(HEAD_START_NS)

    for k in range(2):
        for weight in range(3):
            for way in range(2):
                need(weight, sign[way] * distance(k))
                send_sum(way, k, weight).start()

    def add(way, k, weight):
        offset, which = sign[way] * (distance(k) - 1), layer(way, k)
        base = block(weight, offset)

        def body(r, c, carry):
            term = own[weight][which, pl.ds(pl.multiple_of(base + r, ROWS), ROWS), c].astype(F32)
            so_far = arrived[weight][way, k, pl.ds(r, ROWS), c].astype(F32)
            arrived[weight][way, k, pl.ds(r, ROWS), c] = (so_far + term).astype(BF16)
            return carry

        pieces(rows[weight], cols[weight], body, 0)

    for k in range(sends - 2):
        for weight in range(3):
            for way in range(2):
                need(weight, sign[way] * (distance(k) - 1))
                send_sum(way, k, weight).wait_recv()
                add(way, k, weight)
            for way in range(2):
                send_sum(way, k + 2, weight).start()
            for way in range(2):
                send_sum(way, k, weight).wait_send()

    def finish(which, weight, sums):
        base = block(weight, 0)
        first, second = ((way, k) for way in range(2) for k in (sends - 2, sends - 1) if layer(way, k) == which)

        def body(r, c, sums):
            g = own[weight][which, pl.ds(pl.multiple_of(base + r, ROWS), ROWS), c].astype(F32)
            g += arrived[weight][first[0], first[1], pl.ds(r, ROWS), c].astype(F32)
            g += arrived[weight][second[0], second[1], pl.ds(r, ROWS), c].astype(F32)
            g = g.astype(BF16)
            total[weight][which, pl.ds(r, ROWS), c] = g
            g = g.astype(F32)
            g = g * g
            return sums + (g[:8] + g[8:])

        return pieces(rows[weight], cols[weight], body, sums)

    for weight in range(3):
        need(weight, 0)
        for way in range(2):
            send_sum(way, sends - 2, weight).wait_recv()
    sums = jnp.zeros((8, LANES), F32)
    for weight in range(3):
        for way in range(2):
            send_sum(way, sends - 1, weight).wait_recv()
            sums = finish(layer(way, sends - 1), weight, sums)
    sums = sum(sums[:, c : c + 128] for c in range(0, LANES, 128))
    squares[0] = jnp.broadcast_to(jnp.sum(sums, axis=0, keepdims=True), (8, 128))

    def send_squares(offset):
        return pltpu.make_async_remote_copy(
            src_ref=squares.at[0],
            dst_ref=squares.at[offset],
            send_sem=sq_send.at[offset],
            recv_sem=sq_recv.at[offset],
            device_id={"dp": at(offset)},
            device_id_type=MESH,
        )

    far_first = sorted(range(1, n), key=lambda offset: -min(offset, n - offset))
    for weight in range(3):
        for which in range(3):
            state(which, weight).wait()
    for offset in far_first:
        send_squares(offset).start()
    for weight in range(3):
        for way in range(2):
            for k in range(sends - 2, sends):
                send_sum(way, k, weight).wait_send()
    everyone = squares[0, :1]
    for offset in reversed(far_first):
        send_squares(offset).wait_recv()
        everyone += squares[offset, :1]
    everyone = jnp.sum(everyone, axis=1, keepdims=True)
    factor[...] = jnp.broadcast_to(jnp.minimum(1.0, 0.5 * lax.rsqrt(everyone / count + 1e-30)), factor.shape)

    for offset in far_first:
        send_squares(offset).wait_send()


def adamw(*refs):
    total, w_old, m, v = (refs[i : i + 3] for i in (0, 3, 6, 9))
    factor = refs[12][:1, :1]
    w_new, m_out, v_out = (refs[i : i + 3] for i in (13, 16, 19))
    m_new, v_new = refs[23:26], refs[26:29]
    sem = refs[29]
    copies = []
    for which in range(2):
        for weight in range(3):

            def body(r, c, carry, which=which, weight=weight):
                part = (which, pl.ds(r, ROWS), c)
                g = total[weight][part].astype(F32) * factor
                w = w_old[weight][part].astype(F32)
                moment = 0.9 * m[weight][part] + 0.1 * g
                second = 0.95 * v[weight][part] + 0.05 * g * g
                m_new[weight][part] = moment
                v_new[weight][part] = second
                step = moment * lax.rsqrt(second + 1e-8) + 0.1 * w
                w_new[weight][part] = (w - 0.02 * step).astype(BF16)
                return carry

            pieces(m[weight].shape[1], m[weight].shape[2], body, 0)
            for i, (source, target) in enumerate(((m_new, m_out), (v_new, v_out))):
                copy = pltpu.make_async_copy(source[weight].at[which], target[weight].at[which], sem.at[i, which, weight])
                copy.start()
                copies.append(copy)
    for copy in copies:
        copy.wait()


def gather(n, first, last, *refs):
    count = (len(refs) - 3) // 2
    before, whole = refs[:count], refs[count + 1 : 2 * count + 1]
    sends, recvs = refs[2 * count + 1 :]
    half = n // 2
    me = lax.axis_index("dp")
    sign = (1, -1)

    def at(offset):
        return lax.rem(me + offset + n, n)

    barrier = pltpu.get_barrier_semaphore()
    for offset in sign:
        pl.semaphore_signal(barrier, inc=1, device_id={"dp": at(offset)}, device_id_type=MESH)
    pl.semaphore_wait(barrier, 2)

    def copy(way, q, which, weight, behind):
        rows = whole[weight].shape[1] // n
        part = (which, pl.ds(pl.multiple_of(at(-sign[way] * behind) * rows, rows), rows))
        if behind == 0:
            source = before[weight].at[which]
        else:
            source = (before if behind == first else whole)[weight].at[part]
        return pltpu.make_async_remote_copy(
            src_ref=source,
            dst_ref=whole[weight].at[part],
            send_sem=sends.at[way, q - first, which, weight],
            recv_sem=recvs.at[way, q - first, which, weight],
            device_id={"dp": at(sign[way])},
            device_id_type=MESH,
        )

    def goes(way, q, which):
        return q < half - 1 or which == way

    def keep(which, weight):
        rows, cols = before[weight].shape[1:]

        def body(r, c, carry):
            whole[weight][which, pl.ds(pl.multiple_of(me * rows + r, ROWS), ROWS), c] = before[weight][which, pl.ds(r, ROWS), c]
            return carry

        pieces(rows, cols, body, 0)

    each = [(which, weight) for which in range(2) for weight in range(count)]
    for q in range(first, last + 1):
        for nth, weight in each:
            for way in range(2):
                which = (nth + way) % 2
                if q > first and goes(way, q - 1, which):
                    copy(way, q - 1, which, weight, q).wait_recv()
                if q < last and goes(way, q, which):
                    copy(way, q, which, weight, q).start()
                if q > first + 1:
                    copy(way, q - 2, which, weight, q - 2).wait_send()
        if q == 0:
            for which, weight in each:
                keep(which, weight)
    for which, weight in each:
        for way in range(2):
            if goes(way, last - 1, which):
                copy(way, last - 1, which, weight, last - 1).wait_send()


def put_out(n, offsets, *refs):
    whole, out, sem = refs[:3], refs[-5:-2], refs[-1]
    me = lax.axis_index("dp")
    copies = []
    for i in range(3):
        rows = whole[i].shape[1] // n
        for j, offset in enumerate(offsets):
            part = pl.ds(pl.multiple_of(lax.rem(me + offset, n) * rows, rows), rows)
            copies.append(pltpu.make_async_copy(whole[i].at[:, part], out[i].at[:, part], sem.at[i, j]))
    for copy in copies:
        copy.start()
    for copy in copies:
        copy.wait()


def solution(mesh):
    n = mesh.shape["dp"]

    def step(*arrays):
        terms, weights, m, v = (arrays[i : i + 3] for i in (0, 3, 6, 9))
        terms = tuple(t[0] for t in terms)
        half = n // 2
        shapes = [one.shape for one in m]
        dma = pltpu.SemaphoreType.DMA
        scratch = [pltpu.VMEM(t.shape, t.dtype) for t in terms]
        scratch += [pltpu.VMEM((2, n - 1, *s[1:]), BF16) for s in shapes]
        scratch += [
            pltpu.VMEM((n, 8, 128), F32),
            dma((3, n)),
            dma((3, 3)),
            dma((2, n - 1, 3)),
            dma((2, n - 1, 3)),
            dma((n,)),
            dma((n,)),
        ]
        hbm, vmem, anywhere = (pl.BlockSpec(memory_space=space) for space in (pltpu.HBM, pltpu.VMEM, pl.ANY))

        def in_vmem(arrays):
            return [pltpu.with_memory_space_constraint(one, pltpu.VMEM) for one in arrays]

        token = jax.ShapeDtypeStruct((8, 128), F32)
        limit = pltpu.CompilerParams(vmem_limit_bytes=2**20, has_side_effects=True)

        def gathered(before, first, last, after, collective_id):
            return pl.pallas_call(
                functools.partial(gather, n, first, last),
                out_shape=[pltpu.VMEM(one.shape, one.dtype) for one in weights],
                in_specs=[vmem] * 3 + [anywhere],
                out_specs=[vmem] * 3,
                scratch_shapes=[dma((2, last - first, 2, 3))] * 2,
                compiler_params=pltpu.CompilerParams(collective_id=collective_id, has_side_effects=True, vmem_limit_bytes=2**20),
            )(*in_vmem(before), after)

        def written(whole, offsets, so_far):
            *out, after = pl.pallas_call(
                functools.partial(put_out, n, offsets),
                out_shape=[*(jax.ShapeDtypeStruct(one.shape, one.dtype) for one in weights), token],
                in_specs=[vmem] * 3 + [anywhere] * len(so_far),
                out_specs=[anywhere] * 4,
                scratch_shapes=[dma((3, len(offsets)))],
                input_output_aliases={3 + i: i for i in range(len(so_far))},
                compiler_params=limit,
            )(*in_vmem(whole), *so_far)
            return out, after

        in_hbm = [pltpu.with_memory_space_constraint(one, pltpu.HBM) for one in (*terms, *weights, *m, *v)]
        results = [(s, BF16) for s in shapes] * 2 + [(s, F32) for s in shapes] * 2 + [((8, 128), F32)]
        summed = pl.pallas_call(
            functools.partial(reduce_and_norm, n),
            out_shape=[pltpu.VMEM(*one) for one in results],
            in_specs=[hbm] * len(in_hbm),
            out_specs=[vmem] * len(results),
            scratch_shapes=scratch,
            compiler_params=pltpu.CompilerParams(collective_id=0, has_side_effects=True, vmem_limit_bytes=20 * 2**20),
        )(*in_hbm)
        *new, after = pl.pallas_call(
            adamw,
            out_shape=[pltpu.VMEM(s, BF16) for s in shapes] + [jax.ShapeDtypeStruct(s, F32) for s in shapes] * 2 + [token],
            in_specs=[vmem] * len(summed),
            out_specs=[vmem] * 3 + [anywhere] * 7,
            scratch_shapes=[pltpu.VMEM(s, F32) for s in shapes] * 2 + [dma((2, 2, 3))],
            compiler_params=pltpu.CompilerParams(vmem_limit_bytes=6 * 2**20, has_side_effects=True),
        )(*in_vmem(summed))
        blocks, state = new[:3], new[3:]
        near = gathered(blocks, 0, NEAR, after, 1)
        out, after = written(near, [offset % n for offset in range(-NEAR, NEAR + 1)], ())
        far = gathered(near, NEAR, half, after, 2)
        out, _ = written(far, range(NEAR + 1, n - NEAR), out)
        return (*out, *state)

    all_of, cut = P(None, None, None), P(None, "dp", None)
    return jax.shard_map(
        step,
        mesh=mesh,
        in_specs=(P(("rep", "dp"), None, None, None),) * 3 + (all_of,) * 3 + (cut,) * 6,
        out_specs=(P("rep", None, None),) * 3 + (P("rep", "dp", None),) * 6,
        check_vma=False,
    )
```
